32 devices in a mesh: dp: 16 (over z, y, x), shard: 2 (over core).
Axes of the slice: x: 2, y: 2, z: 4, core: 2. Of those that a mesh axis runs over, the one named last changes fastest.
Arguments:
- features: bfloat16 [65536, 1024], P('dp'), may hold values from -150 to 150
- shared_weight: bfloat16 [1024, 2048], P(None, 'shard'), may hold values from -0.1875 to 0.1875
- task_heads: bfloat16 [6, 2048], P(None, 'shard'), may hold values from -0.4 to 0.4
- labels: int32 [65536, 6], P('dp'), may hold values from 0 to 1
- task_masks: int32 [65536, 6], P('dp'), may hold values from 0 to 1
- task_weights: float32 [6], replicated, may hold values from 0.5 to 2
- initial_losses: float32 [6], replicated, may hold values from 0.2 to 1
Outputs:
- update: float32 [1024, 2048], P('dp', 'shard')
- new_weights: float32 [6], replicated
The draws below stay inside these ranges and needn't reach their ends.
All inputs are finite; a program needn't handle non-finite values.
Results may differ from the reference program's by a relative error of at most 0.00089.
Values sent between devices are 32-bit elements; how exact they have to be, the bound alone decides.
A program may use at most 256 MiB of HBM per device.

```python
import math
import jax
import jax.numpy as jnp
from jax import lax

DIN = 1024
DH = 2048
TASKS = 6
SAMPLES_DEV = 4096
SAMPLES = 65536
N_DP = 16


def draw_features(key, part):
    subkeys = jax.random.split(key, 3)
    total_rows = SAMPLES_DEV * N_DP
    row_ids = jnp.arange(total_rows)
    column_ids = jnp.arange(DIN)
    roughness = jax.random.uniform(subkeys[1], (DIN,), jnp.float32, -0.5, 0.5)
    column_scale = jnp.exp(math.log(3.0) * column_ids.astype(jnp.float32) / (DIN - 1) + math.log(4.0) * roughness)
    pairing = jax.random.permutation(subkeys[2], N_DP)
    spike_gain = jnp.where(pairing[row_ids // SAMPLES_DEV][:, None] == (column_ids // (DIN // N_DP))[None, :], 3.0, 1.0)
    base_draw = jax.random.truncated_normal(subkeys[0], -4.0, 4.0, (total_rows, DIN), jnp.float32)
    return (base_draw * column_scale[None, :] * spike_gain).astype(jnp.bfloat16)


def draw_task_heads(key, part):
    subkeys = jax.random.split(key, 2)
    column_ids = jnp.arange(DH).astype(jnp.float32)
    roughness = jax.random.uniform(subkeys[1], (DH,), jnp.float32, -0.5, 0.5)
    column_scale = jnp.exp(math.log(3.0) * column_ids / (DH - 1) + math.log(2.0) * roughness)
    base_draw = jax.random.truncated_normal(subkeys[0], -4.0, 4.0, (TASKS, DH), jnp.float32)
    values = base_draw * column_scale[None, :] / math.sqrt(DH)
    return jnp.clip(values, -0.3984375, 0.3984375).astype(jnp.bfloat16)


def draw_task_masks(key, part):
    total_rows = SAMPLES_DEV * N_DP
    row_ids = jnp.arange(total_rows, dtype=jnp.int32)
    threshold = 250 + 500 * row_ids // (total_rows - 1)
    drawn = jax.random.randint(key, (total_rows, TASKS), 0, 1000, dtype=jnp.int32)
    return (drawn < threshold[:, None]).astype(jnp.int32)


def touch_ends(array, stream_key, smallest, high):
    longest = array.shape.index(max(array.shape))
    spots = []
    for shift in (0, 1):
        where = [jax.random.randint(jax.random.fold_in(stream_key, axis), (), 0, length) for axis, length in enumerate(array.shape)]
        where[longest] = (where[longest] + shift) % array.shape[longest]
        spots.append(tuple(where))
    return array.at[spots[0]].set(smallest).at[spots[1]].set(high)


def shard_levels(key, shape, shards, low, top_value):
    gain, own = 1.0, jax.random.fold_in(key, 6)
    for dim, parts in shards:
        steps = jnp.exp(jax.random.uniform(jax.random.fold_in(own, dim), (parts,), jnp.float32, low / len(shards), top_value / len(shards)))
        gain = gain * jnp.repeat(steps, shape[dim] // parts).reshape([-1 if axis == dim else 1 for axis in range(len(shape))])
    return gain


def gaussian(stream_key, extent, deviation, most, shards=(), held_as=jnp.bfloat16):
    loudness = shard_levels(stream_key, extent, shards, -0.22, 0.18) if shards else 1.0
    values = jax.random.normal(stream_key, extent, jnp.float32) * deviation * loudness
    return jnp.minimum(jnp.maximum(values, -most), most).astype(held_as)


def setup_inputs(seed: int = 0) -> dict:
    splits = jax.random.split(jax.random.key(seed), 8)
    features = draw_features(jax.random.fold_in(splits[7], 71), 0)
    shared_weight = gaussian(splits[1], (DIN, DH), DIN ** -0.5, 0.1875, ((1, 2),))
    task_heads = draw_task_heads(jax.random.fold_in(splits[7], 71), 0)
    labels = touch_ends(jax.random.randint(splits[3], (SAMPLES, TASKS), 0, 2), jax.random.fold_in(splits[3], 1), 0, 1).astype(jnp.int32)
    task_masks = draw_task_masks(jax.random.fold_in(splits[7], 71), 0)
    task_weights = jnp.clip(jnp.exp(jax.random.uniform(splits[5], (TASKS,), jnp.float32, math.log(0.5), math.log(2.0))), 0.5, 2.0)
    initial_losses = jnp.clip(jnp.exp(jax.random.uniform(splits[6], (TASKS,), jnp.float32, math.log(0.2), math.log(1.0))), 0.2, 1.0)
    return dict(features=features, shared_weight=shared_weight, task_heads=task_heads, labels=labels, task_masks=task_masks, task_weights=task_weights, initial_losses=initial_losses)


epsilon = 1e-06
learn_rate = 0.5
asymmetry = 1.5

def silu_parts(preact):
    sigmoid_pre = jax.nn.sigmoid(preact)
    return (preact * sigmoid_pre, sigmoid_pre * (1.0 + preact * (1.0 - sigmoid_pre)))

def renew_weights(losses, squares, task_weights, initial_losses, entries):
    root_mean = jnp.sqrt(squares / entries + epsilon)
    scaled = task_weights * root_mean
    average = jnp.mean(scaled)
    loss_ratio = losses / initial_losses
    relative = loss_ratio / jnp.mean(loss_ratio)
    target = average * relative ** asymmetry
    distance = (scaled - target) / average
    raised = task_weights * jnp.exp(-learn_rate * distance)
    return raised.shape[0] * raised / jnp.sum(raised)

def reference(features, shared_weight, task_heads, labels, task_masks, task_weights, initial_losses):
    blocks = features.reshape(N_DP, SAMPLES_DEV, DIN)
    label_blocks = labels.reshape(N_DP, SAMPLES_DEV, TASKS)
    mask_blocks = task_masks.reshape(N_DP, SAMPLES_DEV, TASKS)
    heads_wide = task_heads.astype(jnp.float32)

    def block_step(running, inputs):
        grad_sum, loss_sum = running
        rows_in, label_rows, mask_rows = inputs
        preact = jnp.dot(rows_in, shared_weight, preferred_element_type=jnp.float32)
        activated, silu_slope = silu_parts(preact)
        hidden = activated.astype(jnp.bfloat16)
        logits = jnp.dot(hidden, task_heads.T, preferred_element_type=jnp.float32)
        targets = label_rows.astype(jnp.float32)
        mask_float = mask_rows.astype(jnp.float32)
        loss_sum = loss_sum + lax.optimization_barrier(jnp.sum(mask_float * (jax.nn.softplus(logits) - targets * logits), axis=0))
        errors = mask_float * (jax.nn.sigmoid(logits) - targets)
        back_terms = (errors[:, :, None] * silu_slope[:, None, :] * heads_wide[None]).astype(jnp.bfloat16)
        back_flat = back_terms.reshape(SAMPLES_DEV, TASKS * DH)
        grad_sum = grad_sum + lax.dot_general(rows_in, back_flat, (((0,), (0,)), ((), ())), preferred_element_type=jnp.float32)
        return ((grad_sum, loss_sum), None)
    start_state = (jnp.zeros((DIN, TASKS * DH), jnp.float32), jnp.zeros((TASKS,), jnp.float32))
    (grad_sum, loss_sum), unused = lax.scan(block_step, start_state, (blocks, label_blocks, mask_blocks))
    gradients = grad_sum.reshape(DIN, TASKS, DH)
    losses = loss_sum / SAMPLES
    squares = lax.optimization_barrier(jnp.sum(gradients * gradients, axis=(0, 2)))
    new_weights = renew_weights(losses, squares, task_weights, initial_losses, DIN * DH)
    combined = jnp.einsum('t,rtc->rc', new_weights, gradients, precision=lax.Precision.HIGHEST)
    update = combined * lax.rsqrt(jnp.mean(combined * combined) + epsilon)
    return (update, new_weights)
```

```python
import jax
import jax.numpy as jnp
from jax import lax
from jax.sharding import PartitionSpec as P

epsilon = 1e-06
learn_rate = 0.5
asymmetry = 1.5


def silu_parts(preact):
    sigmoid_pre = jax.nn.sigmoid(preact)
    return (preact * sigmoid_pre, sigmoid_pre * (1.0 + preact * (1.0 - sigmoid_pre)))


def renew_weights(losses, squares, task_weights, initial_losses, entries):
    root_mean = jnp.sqrt(squares / entries + epsilon)
    scaled = task_weights * root_mean
    average = jnp.mean(scaled)
    loss_ratio = losses / initial_losses
    relative = loss_ratio / jnp.mean(loss_ratio)
    target = average * relative**asymmetry
    distance = (scaled - target) / average
    raised = task_weights * jnp.exp(-learn_rate * distance)
    return raised.shape[0] * raised / jnp.sum(raised)


def task_term(inputs, terms):
    return lax.dot_general(
        inputs, terms, (((0,), (0,)), ((), ())), preferred_element_type=jnp.float32
    )


def quadratic(gram_total, new_weights):
    inner = jnp.dot(gram_total, new_weights, precision=lax.Precision.HIGHEST)
    return jnp.dot(new_weights, inner, precision=lax.Precision.HIGHEST)


def exchange_order(task, levels):
    if levels == 4:
        orders = ((0, 1, 3, 2), (1, 0, 2, 3), (2, 1, 0, 3), (3, 0, 1, 2))
        return orders[(0, 1, 2, 3, 0, 1)[task % 6]]
    return tuple((task + level) % levels for level in range(levels))


def halve_rows(term, order, levels, replica_count):
    me = lax.axis_index("dp")
    rows, columns = term.shape
    block = term.reshape((2,) * levels + (rows // replica_count, columns))
    axes = list(range(levels - 1, -1, -1))
    for bit in order:
        axis = axes.index(bit)
        mine = (me >> bit) & 1
        sent = lax.dynamic_index_in_dim(block, 1 - mine, axis, keepdims=False)
        kept = lax.dynamic_index_in_dim(block, mine, axis, keepdims=False)
        pairs = [(device, device ^ (1 << bit)) for device in range(replica_count)]
        block = kept + lax.ppermute(sent, "dp", pairs)
        axes.remove(bit)
    return block


def scatter_rows(term, task, replica_count):
    levels = replica_count.bit_length() - 1
    if (1 << levels) != replica_count:
        return lax.psum_scatter(term, "dp", scatter_dimension=0, tiled=True)
    return halve_rows(term, exchange_order(task, levels), levels, replica_count)


def sum_over_shard(partial, shard_count):
    if shard_count == 2:
        return partial + lax.ppermute(partial, "shard", [(0, 1), (1, 0)])
    return lax.psum(partial, "shard")


def on_device(
    features, shared_weight, task_heads, labels, task_masks, task_weights, initial_losses
):
    shard_count = lax.axis_size("shard")
    replica_count = lax.axis_size("dp")
    sample_count = features.shape[0]
    width_in = features.shape[1]
    local_hidden = shared_weight.shape[1]
    task_count = task_heads.shape[0]
    entries = width_in * local_hidden * shard_count
    total_samples = sample_count * replica_count
    preact = jnp.dot(features, shared_weight, preferred_element_type=jnp.float32)
    activated, silu_slope = silu_parts(preact)
    hidden = activated.astype(jnp.bfloat16)
    partial_logits = lax.dot_general(
        task_heads, hidden, (((1,), (1,)), ((), ())), preferred_element_type=jnp.float32
    )
    logits = sum_over_shard(partial_logits, shard_count)
    targets = labels.T.astype(jnp.float32)
    mask_float = task_masks.T.astype(jnp.float32)
    loss_part = (
        jnp.sum(mask_float * (jax.nn.softplus(logits) - targets * logits), axis=1) / total_samples
    )
    errors = (mask_float * (jax.nn.sigmoid(logits) - targets)).T
    heads_wide = task_heads.astype(jnp.float32)
    pieces = []
    for task in range(task_count):
        terms = (errors[:, task, None] * silu_slope * heads_wide[task][None]).astype(jnp.bfloat16)
        pieces.append(scatter_rows(task_term(features, terms), task, replica_count))
    gram = jnp.stack(
        [jnp.stack([jnp.sum(one * other) for other in pieces]) for one in pieces]
    )
    sums = jnp.concatenate([gram, loss_part[None] / shard_count], axis=0)
    sums = lax.psum(sums, ("dp", "shard"))
    gram_total, losses = sums[:task_count], sums[task_count]
    new_weights = renew_weights(
        losses, jnp.diagonal(gram_total), task_weights, initial_losses, entries
    )
    mean_square = quadratic(gram_total, new_weights) / entries
    combined = new_weights[0] * pieces[0]
    for task in range(1, task_count):
        combined = combined + new_weights[task] * pieces[task]
    update = combined * lax.rsqrt(mean_square + epsilon)
    return (update, new_weights)


def solution(mesh):
    return jax.shard_map(
        on_device,
        mesh=mesh,
        in_specs=(
            P("dp", None),
            P(None, "shard"),
            P(None, "shard"),
            P("dp", None),
            P("dp", None),
            P(),
            P(),
        ),
        out_specs=(P("dp", "shard"), P()),
        check_vma=False,
    )
```
